32 devices in a mesh: section: 16 (over z, x, core), dp: 2 (over y).
Axes of the slice: x: 2, y: 2, z: 4, core: 2. Of those that a mesh axis runs over, the one named last changes fastest.
Arguments:
- w_value: bfloat16 [16, 2, 4608, 1024], P('section', None, None, 'dp'), may hold values from -0.09375 to 0.09375
- w_out: bfloat16 [16, 2, 1024, 4608], P('section', None, 'dp'), may hold values from -0.1875 to 0.1875
- norm_gain: float32 [16, 2, 4608], P('section'), may hold values from 0.5 to 1.5
- saved_inputs: bfloat16 [16, 3, 2, 16, 4608], P('section', None, None, 'dp'), may hold values from -6 to 6
- arriving: bfloat16 [16, 2, 16, 4608], P('section', None, 'dp'), may hold values from -6 to 6
- returning: bfloat16 [16, 2, 16, 4608], P('section', None, 'dp'), may hold values from -6 to 6
- fresh_rows: bfloat16 [4, 16, 4608], P(None, 'dp'), may hold values from -6 to 6
- targets: bfloat16 [4, 16, 4608], P(None, 'dp'), may hold values from -6 to 6
- fill_slots: int32 [16, 4, 2], P('section'), may hold values from 0 to 2
- read_slots: int32 [16, 4, 2], P('section'), may hold values from 0 to 2
Outputs:
- activ_out: bfloat16 [16, 2, 16, 4608], P('section', None, 'dp')
- cotan_out: bfloat16 [16, 2, 16, 4608], P('section', None, 'dp')
- stash_out: bfloat16 [16, 3, 2, 16, 4608], P('section', None, None, 'dp')
- grad_value: bfloat16 [16, 2, 4608, 1024], P('section', None, None, 'dp')
- grad_out: bfloat16 [16, 2, 1024, 4608], P('section', None, 'dp')
- grad_gain: float32 [16, 2, 4608], P('section')
The draws below stay inside these ranges and needn't reach their ends.
All inputs are finite; a program needn't handle non-finite values.
Results may differ from the reference program's by a relative error of at most 0.029.
Values may be sent and summed in bfloat16 or wider, within the bound.
No kernel may reach another device: no remote copies, remote signals or barrier semaphores. Data moves between devices by JAX's collectives and lax.ppermute only.
A program may use at most 192 MiB of HBM per device.

```python
import jax
import jax.numpy as jnp
from jax import lax

D = 4608
K = 1024
TICKS = 4
SLOTS = 3
ROWS = 16
N_SECTION = 16
N_DP = 2


def set_ends(drawn, stream_key, smallest, top_value):
    extent = drawn.shape
    place = [jax.random.randint(jax.random.fold_in(stream_key, axis), (), 0, extent[axis]) for axis in range(len(extent))]
    drawn = drawn.at[tuple(place)].set(smallest)
    longest = extent.index(max(extent))
    place[longest] = (place[longest] + 1) % extent[longest]
    return drawn.at[tuple(place)].set(top_value)


def block_scale(rng, dims, cuts, low, high):
    gain, own = 1.0, jax.random.fold_in(rng, 6)
    for position, shards_of in cuts:
        steps = jnp.exp(jax.random.uniform(jax.random.fold_in(own, position), (shards_of,), jnp.float32, low / len(cuts), high / len(cuts)))
        gain = gain * jnp.repeat(steps, dims[position] // shards_of).reshape([-1 if axis == position else 1 for axis in range(len(dims))])
    return gain


def scatter_about(key, shape, deviation, reach, cuts=(), held_as=jnp.bfloat16):
    values = jax.random.normal(key, shape, jnp.float32) * deviation
    if len(cuts) > 0:
        values = block_scale(key, shape, cuts, -0.22, 0.18) * values
    return jnp.clip(values, min=-reach, max=reach).astype(held_as)


def setup_inputs(seed: int = 0) -> dict:
    key_of = jax.random.split(jax.random.key(seed), 11)
    w_value = scatter_about(key_of[0], (N_SECTION, 2, D, K), D ** -0.5, 0.09375, ((0, 16), (3, 2)))
    w_out = scatter_about(key_of[1], (N_SECTION, 2, K, D), K ** -0.5, 0.1875, ((0, 16), (2, 2)))
    norm_gain = jnp.clip(1.0 + 0.1 * jax.random.normal(key_of[2], (N_SECTION, 2, D), jnp.float32), 0.5, 1.5)
    saved_inputs = scatter_about(key_of[3], (N_SECTION, SLOTS, 2, ROWS, D), 1.0, 6.0, ((0, 16), (3, 2)))
    arriving = scatter_about(key_of[4], (N_SECTION, 2, ROWS, D), 1.0, 6.0, ((0, 16), (2, 2)))
    returning = scatter_about(key_of[5], (N_SECTION, 2, ROWS, D), 1.0, 6.0, ((0, 16), (2, 2)))
    fresh_rows = scatter_about(key_of[6], (TICKS, ROWS, D), 1.0, 6.0, ((1, 2),))
    targets = scatter_about(key_of[7], (TICKS, ROWS, D), 1.0, 6.0, ((1, 2),))
    fill_slots = set_ends(jax.random.randint(key_of[8], (N_SECTION, TICKS, 2), 0, SLOTS), jax.random.fold_in(key_of[8], 1), 0, SLOTS - 1).astype(jnp.int32)
    read_slots = set_ends(jax.random.randint(key_of[9], (N_SECTION, TICKS, 2), 0, SLOTS), jax.random.fold_in(key_of[9], 1), 0, SLOTS - 1).astype(jnp.int32)
    return dict(w_value=w_value, w_out=w_out, norm_gain=norm_gain, saved_inputs=saved_inputs, arriving=arriving, returning=returning, fresh_rows=fresh_rows, targets=targets, fill_slots=fill_slots, read_slots=read_slots)


epsilon = 1e-06

def exact_dot(left, right):
    return jnp.dot(left.astype(jnp.float32), right.astype(jnp.float32), precision=lax.Precision.HIGHEST)

def normalize(block_rows, gain_row):
    values = block_rows.astype(jnp.float32)
    inv_root = lax.rsqrt(lax.optimization_barrier(jnp.mean(values * values, axis=-1, keepdims=True)) + epsilon)
    scaled = values * inv_root
    return (scaled, inv_root, (scaled * gain_row).astype(jnp.bfloat16))

def shard_sums(left, right):
    pieces = right.shape[0] // N_DP
    split_left = left.astype(jnp.float32).reshape(left.shape[0], N_DP, pieces)
    split_right = right.astype(jnp.float32).reshape(N_DP, pieces, right.shape[1])
    terms = jnp.einsum('rjk,jkd->jrd', split_left, split_right, precision=lax.Precision.HIGHEST)
    rounded = lax.optimization_barrier(terms.astype(jnp.bfloat16))
    return lax.optimization_barrier(jnp.sum(rounded.astype(jnp.float32), axis=0))

def forward_layer(block_rows, gain_row, value_mat, out_mat):
    scaled, inv_root, normed = normalize(block_rows, gain_row)
    values = exact_dot(normed, value_mat).astype(jnp.bfloat16)
    return (block_rows.astype(jnp.float32) + shard_sums(values, out_mat)).astype(jnp.bfloat16)

def backward_layer(source, upstream, gain_row, value_mat, out_mat):
    scaled, inv_root, normed = normalize(source, gain_row)
    down_grad = exact_dot(upstream, out_mat.T).astype(jnp.bfloat16)
    pulled = shard_sums(down_grad, value_mat.T)
    weighted = pulled * gain_row
    inner_mean = lax.optimization_barrier(jnp.mean(weighted * scaled, axis=-1, keepdims=True))
    grad_in = (upstream.astype(jnp.float32) + inv_root * (weighted - scaled * inner_mean)).astype(jnp.bfloat16)
    values = exact_dot(normed, value_mat).astype(jnp.bfloat16)
    return (grad_in, exact_dot(normed.T, down_grad), exact_dot(values.T, upstream), lax.optimization_barrier(jnp.sum(pulled * scaled, axis=0)))

def section_work(entries):
    inputs_now, upstream_now, sources, gains, value_mats, out_mats = entries
    layer_outs, grad_ins, value_terms, out_terms, gain_terms = ([], [], [], [], [])
    for group in range(2):
        layer_outs.append(forward_layer(inputs_now[group], gains[group], value_mats[group], out_mats[group]))
        grad_in, value_term, out_term, gain_term = backward_layer(sources[group], upstream_now[group], gains[group], value_mats[group], out_mats[group])
        grad_ins.append(grad_in)
        value_terms.append(value_term)
        out_terms.append(out_term)
        gain_terms.append(gain_term)
    return (jnp.stack(layer_outs), jnp.stack(grad_ins), jnp.stack(value_terms), jnp.stack(out_terms), jnp.stack(gain_terms))

def reference(w_value, w_out, norm_gain, saved_inputs, arriving, returning, fresh_rows, targets, fill_slots, read_slots):
    activations = arriving
    cotangents = returning
    saved = saved_inputs
    value_sums = jnp.zeros(w_value.shape, jnp.float32)
    out_sums = jnp.zeros(w_out.shape, jnp.float32)
    gain_sums = jnp.zeros(norm_gain.shape, jnp.float32)
    slot_ids = jnp.arange(SLOTS, dtype=jnp.int32)
    outputs = activations
    gradients = cotangents
    for tick_index in range(TICKS):
        if tick_index > 0:
            lower_group = jnp.concatenate([fresh_rows[tick_index][None], outputs[:-1, 0]], axis=0)
            upper_group = jnp.concatenate([outputs[-1:, 0], outputs[:-1, 1]], axis=0)
            activations = jnp.stack([lower_group, upper_group], axis=1)
            finish = (outputs[-1, 1].astype(jnp.float32) - targets[tick_index - 1].astype(jnp.float32)).astype(jnp.bfloat16)
            lower_grad = jnp.concatenate([gradients[1:, 0], gradients[:1, 1]], axis=0)
            upper_grad = jnp.concatenate([gradients[1:, 1], finish[None]], axis=0)
            cotangents = jnp.stack([lower_grad, upper_grad], axis=1)
        written = slot_ids[None, :, None] == fill_slots[:, tick_index, :][:, None, :]
        saved = jnp.where(written[:, :, :, None, None], activations[:, None], saved)
        chosen = slot_ids[None, :, None] == read_slots[:, tick_index, :][:, None, :]
        sources = lax.optimization_barrier(jnp.sum(jnp.where(chosen[:, :, :, None, None], saved.astype(jnp.float32), jnp.zeros((), jnp.float32)), axis=1)).astype(jnp.bfloat16)
        outputs, gradients, value_terms, out_terms, gain_terms = lax.map(section_work, (activations, cotangents, sources, norm_gain, w_value, w_out))
        value_sums = value_sums + value_terms
        out_sums = out_sums + out_terms
        gain_sums = gain_sums + gain_terms
    grad_scale = (TICKS * ROWS) ** (-0.5)
    return (outputs, gradients, saved, (value_sums * grad_scale).astype(jnp.bfloat16), (out_sums * grad_scale).astype(jnp.bfloat16), gain_sums * grad_scale)
```

```python
import functools

import jax
import jax.numpy as jnp
from jax import lax
from jax.experimental import pallas as pl
from jax.experimental.pallas import tpu as pltpu
from jax.sharding import PartitionSpec as P

epsilon = 1e-06
CHUNKS = 4
GROUPS_PER_CALL = 2


def shifted(shard, axis, by):
    devices = lax.axis_size(axis)
    return lax.ppermute(shard, axis, [(i, (i + by) % devices) for i in range(devices)])


def replicas_of_section(shard, section):
    replicas = lax.axis_size("dp")
    own = lax.axis_index("dp")
    pieces = [shard]
    for by in range(1, replicas):
        pairs = [
            (section * replicas + i, section * replicas + (i + by) % replicas)
            for i in range(replicas)
        ]
        pieces.append(lax.ppermute(shard, ("section", "dp"), pairs))
    return in_order(pieces, own)


def in_order(pieces, own):
    replicas = len(pieces)
    ordered = []
    for target in range(replicas):
        chosen = pieces[0]
        for by in range(1, replicas):
            chosen = jnp.where((own - by) % replicas == target, pieces[by], chosen)
        ordered.append(chosen)
    return jnp.concatenate(ordered, axis=-2)


def all_replicas(shard):
    replicas = lax.axis_size("dp")
    pieces = [shard] + [shifted(shard, "dp", by) for by in range(1, replicas)]
    return in_order(pieces, lax.axis_index("dp"))


def replica_sum(part):
    total = part.astype(jnp.float32)
    for by in range(1, lax.axis_size("dp")):
        total = total + shifted(part, "dp", by).astype(jnp.float32)
    return total


def scaled_rows(block_rows):
    values = block_rows.astype(jnp.float32)
    inv_root = lax.rsqrt(jnp.mean(values * values, axis=-1, keepdims=True) + epsilon)
    return values * inv_root, inv_root


def times_transposed(left, right):
    return lax.dot_general(
        left, right, (((1,), (1,)), ((), ())), preferred_element_type=jnp.float32
    )


def transposed_times(left, right):
    return lax.dot_general(
        left, right, (((0,), (0,)), ((), ())), preferred_element_type=jnp.float32
    )


def weight_copies(first, group, value_hbm, out_hbm, value_vmem, out_vmem, sems):
    step = value_vmem.shape[1] // CHUNKS
    groups = value_vmem.shape[0]
    value, out = [], []
    for c in range(CHUNKS):
        span = pl.ds(c * step, step)
        for g in range(groups):
            value.append(
                pltpu.make_async_copy(
                    value_hbm.at[first + g, span, :], value_vmem.at[g, span, :], sems.at[0, g, c]
                )
            )
            out.append(
                pltpu.make_async_copy(
                    out_hbm.at[first + g, :, span], out_vmem.at[g, :, span], sems.at[1, g, c]
                )
            )
    return value, out


def forward_kernel(first, rows_ref, gain_ref, value_hbm, out_hbm, part_ref, value_vmem, out_vmem, sems):
    groups = value_vmem.shape[0]
    step = value_vmem.shape[1] // CHUNKS
    value_copies, out_copies = weight_copies(
        first, None, value_hbm, out_hbm, value_vmem, out_vmem, sems
    )
    for g in range(groups):
        for copies in (value_copies, out_copies):
            for c in range(CHUNKS):
                copies[c * groups + g].start()
    for g in range(groups):
        scaled, inv_root = scaled_rows(rows_ref[g])
        normed = (scaled * gain_ref[g]).astype(jnp.bfloat16)
        total = jnp.zeros((normed.shape[0], value_vmem.shape[2]), jnp.float32)
        for c in range(CHUNKS):
            value_copies[c * groups + g].wait()
            low = c * step
            total = total + jnp.dot(
                normed[:, low : low + step],
                value_vmem[g, low : low + step, :],
                preferred_element_type=jnp.float32,
            )
        values = total.astype(jnp.bfloat16)
        for c in range(CHUNKS):
            out_copies[c * groups + g].wait()
            low = c * step
            part_ref[g, :, low : low + step] = jnp.dot(
                values, out_vmem[g, :, low : low + step], preferred_element_type=jnp.float32
            ).astype(jnp.bfloat16)


def backward_kernel(
    first, rows_ref, upstream_ref, gain_ref, value_hbm, out_hbm,
    part_ref, normed_ref, down_ref, values_ref, value_vmem, out_vmem, sems,
):
    groups = value_vmem.shape[0]
    step = value_vmem.shape[1] // CHUNKS
    value_copies, out_copies = weight_copies(
        first, None, value_hbm, out_hbm, value_vmem, out_vmem, sems
    )
    for g in range(groups):
        for copies in (out_copies, value_copies):
            for c in range(CHUNKS):
                copies[c * groups + g].start()
    for g in range(groups):
        scaled, inv_root = scaled_rows(rows_ref[g])
        normed = (scaled * gain_ref[g]).astype(jnp.bfloat16)
        normed_ref[g] = normed
        upstream = upstream_ref[g]
        total = jnp.zeros((normed.shape[0], value_vmem.shape[2]), jnp.float32)
        for c in range(CHUNKS):
            out_copies[c * groups + g].wait()
            low = c * step
            total = total + times_transposed(
                upstream[:, low : low + step], out_vmem[g, :, low : low + step]
            )
        down = total.astype(jnp.bfloat16)
        down_ref[g] = down
        total = jnp.zeros_like(total)
        for c in range(CHUNKS):
            value_copies[c * groups + g].wait()
            low = c * step
            piece = value_vmem[g, low : low + step, :]
            total = total + jnp.dot(
                normed[:, low : low + step], piece, preferred_element_type=jnp.float32
            )
            part_ref[g, :, low : low + step] = times_transposed(down, piece).astype(jnp.bfloat16)
        values_ref[g] = total.astype(jnp.bfloat16)


def gradient_kernel(scale, ticks, *refs):
    def joined(some):
        return jnp.concatenate([ref[0] for ref in some], axis=0)

    normed = joined(refs[:ticks])
    upstream = joined(refs[ticks : 2 * ticks])
    down = joined(refs[2 * ticks : 3 * ticks])
    values = joined(refs[3 * ticks : 4 * ticks])
    value_ref, out_ref = refs[4 * ticks :]
    value_ref[0] = (transposed_times(normed, down) * scale).astype(jnp.bfloat16)
    out_ref[0] = (transposed_times(values, upstream) * scale).astype(jnp.bfloat16)


def layer_scratch(groups, value_mats, out_mats):
    return [
        pltpu.VMEM((groups,) + value_mats.shape[1:], value_mats.dtype),
        pltpu.VMEM((groups,) + out_mats.shape[1:], out_mats.dtype),
        pltpu.SemaphoreType.DMA((2, groups, CHUNKS)),
    ]


vmem_spec = pl.BlockSpec(memory_space=pltpu.VMEM)
any_spec = pl.BlockSpec(memory_space=pl.ANY)


def forward_parts(first, rows, gains, value_mats, out_mats):
    groups = rows.shape[0]
    return pl.pallas_call(
        functools.partial(forward_kernel, first),
        out_shape=jax.ShapeDtypeStruct(rows.shape, jnp.bfloat16),
        in_specs=[vmem_spec, vmem_spec, any_spec, any_spec],
        out_specs=vmem_spec,
        scratch_shapes=layer_scratch(groups, value_mats, out_mats),
        cost_estimate=pl.CostEstimate(
            flops=4 * rows.size * value_mats.shape[2],
            bytes_accessed=4 * groups * value_mats.shape[1] * value_mats.shape[2],
            transcendentals=0,
        ),
        name="forward_parts",
    )(rows, gains, value_mats, out_mats)


def backward_parts(first, rows, upstream, gains, value_mats, out_mats):
    groups, row_count = rows.shape[:2]
    small = jax.ShapeDtypeStruct((groups, row_count, value_mats.shape[2]), jnp.bfloat16)
    large = jax.ShapeDtypeStruct(rows.shape, jnp.bfloat16)
    return pl.pallas_call(
        functools.partial(backward_kernel, first),
        out_shape=(large, large, small, small),
        in_specs=[vmem_spec, vmem_spec, vmem_spec, any_spec, any_spec],
        out_specs=(vmem_spec,) * 4,
        scratch_shapes=layer_scratch(groups, value_mats, out_mats),
        cost_estimate=pl.CostEstimate(
            flops=6 * rows.size * value_mats.shape[2],
            bytes_accessed=4 * groups * value_mats.shape[1] * value_mats.shape[2],
            transcendentals=0,
        ),
        name="backward_parts",
    )(rows, upstream, gains, value_mats, out_mats)


def weight_gradients(scale, normed, upstream, down, values):
    ticks = len(normed)
    groups, row_count, width = normed[0].shape
    features = down[0].shape[2]
    step = width // CHUNKS
    wide = pl.BlockSpec((1, row_count, step), lambda g, c: (g, 0, c))
    narrow = pl.BlockSpec((1, row_count, features), lambda g, c: (g, 0, 0))
    return pl.pallas_call(
        functools.partial(gradient_kernel, scale, ticks),
        grid=(groups, CHUNKS),
        out_shape=(
            jax.ShapeDtypeStruct((groups, width, features), jnp.bfloat16),
            jax.ShapeDtypeStruct((groups, features, width), jnp.bfloat16),
        ),
        in_specs=[wide] * (2 * ticks) + [narrow] * (2 * ticks),
        out_specs=(
            pl.BlockSpec((1, step, features), lambda g, c: (g, c, 0)),
            pl.BlockSpec((1, features, step), lambda g, c: (g, 0, c)),
        ),
        cost_estimate=pl.CostEstimate(
            flops=4 * ticks * row_count * groups * width * features,
            bytes_accessed=4 * groups * width * features,
            transcendentals=0,
        ),
        name="weight_gradients",
    )(*normed, *upstream, *down, *values)


def body(
    w_value,
    w_out,
    norm_gain,
    saved_inputs,
    arriving,
    returning,
    fresh_rows,
    targets,
    fill_slots,
    read_slots,
):
    value_mats = w_value[0]
    out_mats = w_out[0]
    gains = norm_gain[0][:, None, :]
    saved = saved_inputs[0]
    fills = fill_slots[0]
    reads = read_slots[0]
    tick_count = fresh_rows.shape[0]
    slot_count = saved.shape[0]
    tok_rows = arriving.shape[2]
    all_rows = tok_rows * lax.axis_size("dp")
    section_index = lax.axis_index("section")
    last_section = lax.axis_size("section") - 1
    row_offset = lax.axis_index("dp") * tok_rows
    calls = [
        (first, slice(first, first + GROUPS_PER_CALL)) for first in range(0, 2, GROUPS_PER_CALL)
    ]

    def own_rows(block):
        return lax.dynamic_slice_in_dim(block, row_offset, tok_rows, block.ndim - 2)

    def read_saved(tick_index):
        return jnp.stack([saved[reads[tick_index, group], group] for group in range(2)])

    inputs = [all_replicas(arriving[0])]
    first_two = all_replicas(jnp.stack([returning[0], read_saved(0)]))
    cotangents, first_source = first_two[0], first_two[1]
    later = all_replicas(jnp.stack([read_saved(t) for t in range(1, tick_count)]))
    old_sources = [first_source] + [later[t] for t in range(tick_count - 1)]
    new_rows = replicas_of_section(fresh_rows[1:], 0)
    ends = replicas_of_section(targets[: tick_count - 1], last_section)

    gain_sums = jnp.zeros((2, gains.shape[2]), jnp.float32)
    kept = [[], [], [], []]
    for tick_index in range(tick_count):
        if tick_index > 0:
            received = shifted(outputs, "section", 1)
            lower_group = jnp.where(section_index == 0, new_rows[tick_index - 1], received[0])
            upper_group = jnp.where(section_index == 0, received[0], received[1])
            inputs.append(jnp.stack([lower_group, upper_group]))
            returned = shifted(gradients, "section", -1)
            finish = (
                outputs[1].astype(jnp.float32) - ends[tick_index - 1].astype(jnp.float32)
            ).astype(jnp.bfloat16)
            cotangents = jnp.stack(
                [
                    jnp.where(section_index == last_section, returned[1], returned[0]),
                    jnp.where(section_index == last_section, finish, returned[1]),
                ]
            )
        activations = inputs[-1]
        forward_part = jnp.concatenate(
            [
                forward_parts(first, activations[span], gains[span], value_mats, out_mats)
                for first, span in calls
            ]
        )
        outputs = (activations.astype(jnp.float32) + replica_sum(forward_part)).astype(
            jnp.bfloat16
        )
        source = old_sources[tick_index]
        for earlier in range(tick_index + 1):
            same = fills[earlier] == reads[tick_index]
            source = jnp.where(same[:, None, None], inputs[earlier], source)
        results = [
            backward_parts(
                first, source[span], cotangents[span], gains[span], value_mats, out_mats
            )
            for first, span in calls
        ]
        backward_part, normed, down, values = [jnp.concatenate(each) for each in zip(*results)]
        for store, item in zip(kept, (normed, cotangents, down, values)):
            store.append(item)
        pulled = replica_sum(backward_part)
        scaled, inv_root = scaled_rows(source)
        weighted = pulled * gains
        inner_mean = jnp.mean(weighted * scaled, axis=-1, keepdims=True)
        gradients = (
            cotangents.astype(jnp.float32) + inv_root * (weighted - scaled * inner_mean)
        ).astype(jnp.bfloat16)
        gain_sums = gain_sums + jnp.sum(pulled * scaled, axis=1)
    grad_scale = (tick_count * all_rows) ** (-0.5)
    grad_value, grad_out = weight_gradients(grad_scale, *kept)
    slot_ids = jnp.arange(slot_count, dtype=jnp.int32)
    stash = saved
    for tick_index in range(tick_count):
        written = slot_ids[:, None] == fills[tick_index][None, :]
        stash = jnp.where(
            written[:, :, None, None], own_rows(inputs[tick_index])[None], stash
        )
    return (
        own_rows(outputs)[None],
        own_rows(gradients)[None],
        stash[None],
        grad_value[None],
        grad_out[None],
        (gain_sums * grad_scale)[None],
    )


def solution(mesh):
    in_specs = (
        P("section", None, None, "dp"),
        P("section", None, "dp", None),
        P("section", None, None),
        P("section", None, None, "dp", None),
        P("section", None, "dp", None),
        P("section", None, "dp", None),
        P(None, "dp", None),
        P(None, "dp", None),
        P("section", None, None),
        P("section", None, None),
    )
    out_specs = (
        P("section", None, "dp", None),
        P("section", None, "dp", None),
        P("section", None, None, "dp", None),
        P("section", None, None, "dp"),
        P("section", None, "dp", None),
        P("section", None, None),
    )
    return jax.shard_map(body, mesh=mesh, in_specs=in_specs, out_specs=out_specs, check_vma=False)
```

```python
import functools

import jax
import jax.numpy as jnp
from jax import lax
from jax.experimental import pallas as pl
from jax.experimental.pallas import tpu as pltpu
from jax.sharding import PartitionSpec as P

epsilon = 1e-06
CHUNKS = 4


def shifted(shard, axis, by):
    devices = lax.axis_size(axis)
    return lax.ppermute(shard, axis, [(i, (i + by) % devices) for i in range(devices)])


def replicas_of_section(shard, section):
    replicas = lax.axis_size("dp")
    own = lax.axis_index("dp")
    pieces = [shard]
    for by in range(1, replicas):
        pairs = [
            (section * replicas + i, section * replicas + (i + by) % replicas)
            for i in range(replicas)
        ]
        pieces.append(lax.ppermute(shard, ("section", "dp"), pairs))
    return in_order(pieces, own)


def in_order(pieces, own):
    replicas = len(pieces)
    ordered = []
    for target in range(replicas):
        chosen = pieces[0]
        for by in range(1, replicas):
            chosen = jnp.where((own - by) % replicas == target, pieces[by], chosen)
        ordered.append(chosen)
    return jnp.concatenate(ordered, axis=-2)


def all_replicas(shard):
    replicas = lax.axis_size("dp")
    pieces = [shard] + [shifted(shard, "dp", by) for by in range(1, replicas)]
    return in_order(pieces, lax.axis_index("dp"))


def replica_sum(part):
    total = part.astype(jnp.float32)
    for by in range(1, lax.axis_size("dp")):
        total = total + shifted(part, "dp", by).astype(jnp.float32)
    return total


def scaled_rows(block_rows):
    values = block_rows.astype(jnp.float32)
    inv_root = lax.rsqrt(jnp.mean(values * values, axis=-1, keepdims=True) + epsilon)
    return values * inv_root, inv_root


def times_transposed(left, right):
    return lax.dot_general(
        left, right, (((1,), (1,)), ((), ())), preferred_element_type=jnp.float32
    )


def transposed_times(left, right):
    return lax.dot_general(
        left, right, (((0,), (0,)), ((), ())), preferred_element_type=jnp.float32
    )


def weight_copies(value_hbm, out_hbm, value_vmem, out_vmem, sems):
    step = value_vmem.shape[1] // CHUNKS
    groups = value_vmem.shape[0]
    value, out = [], []
    for c in range(CHUNKS):
        span = pl.ds(c * step, step)
        for g in range(groups):
            value.append(
                pltpu.make_async_copy(
                    value_hbm.at[g, span, :], value_vmem.at[g, span, :], sems.at[0, g, c]
                )
            )
            out.append(
                pltpu.make_async_copy(
                    out_hbm.at[g, :, span], out_vmem.at[g, :, span], sems.at[1, g, c]
                )
            )
    return value, out


def forward_kernel(
    first_ref, moved_ref, entering_ref, gain_ref, value_hbm, out_hbm,
    part_ref, rows_ref, value_vmem, out_vmem, sems,
):
    groups = value_vmem.shape[0]
    step = value_vmem.shape[1] // CHUNKS
    value_copies, out_copies = weight_copies(
        value_hbm, out_hbm, value_vmem, out_vmem, sems
    )
    for g in range(groups):
        for copies in (value_copies, out_copies):
            for c in range(CHUNKS):
                copies[c * groups + g].start()
    at_first = first_ref[0] == 1

    @pl.when(at_first)
    def _():
        rows_ref[0] = entering_ref[...]
        rows_ref[1] = moved_ref[0]

    @pl.when(jnp.logical_not(at_first))
    def _():
        rows_ref[...] = moved_ref[...]

    for g in range(groups):
        scaled, inv_root = scaled_rows(rows_ref[g])
        normed = (scaled * gain_ref[g]).astype(jnp.bfloat16)
        total = jnp.zeros((normed.shape[0], value_vmem.shape[2]), jnp.float32)
        for c in range(CHUNKS):
            value_copies[c * groups + g].wait()
            low = c * step
            total = total + jnp.dot(
                normed[:, low : low + step],
                value_vmem[g, low : low + step, :],
                preferred_element_type=jnp.float32,
            )
        values = total.astype(jnp.bfloat16)
        for c in range(CHUNKS):
            out_copies[c * groups + g].wait()
            low = c * step
            part_ref[g, :, low : low + step] = jnp.dot(
                values, out_vmem[g, :, low : low + step], preferred_element_type=jnp.float32
            ).astype(jnp.bfloat16)


def backward_kernel(
    last_ref, moved_ref, output_ref, ends_ref, value_hbm, out_hbm,
    part_ref, upstream_ref, down_ref, value_vmem, out_vmem, sems,
):
    groups = value_vmem.shape[0]
    step = value_vmem.shape[1] // CHUNKS
    value_copies, out_copies = weight_copies(
        value_hbm, out_hbm, value_vmem, out_vmem, sems
    )
    for g in range(groups):
        for copies in (out_copies, value_copies):
            for c in range(CHUNKS):
                copies[c * groups + g].start()
    at_last = last_ref[0] == 1

    @pl.when(at_last)
    def _():
        upstream_ref[0] = moved_ref[1]
        upstream_ref[1] = (
            output_ref[1].astype(jnp.float32) - ends_ref[...].astype(jnp.float32)
        ).astype(jnp.bfloat16)

    @pl.when(jnp.logical_not(at_last))
    def _():
        upstream_ref[...] = moved_ref[...]

    for g in range(groups):
        upstream = upstream_ref[g]
        total = jnp.zeros((upstream.shape[0], value_vmem.shape[2]), jnp.float32)
        for c in range(CHUNKS):
            out_copies[c * groups + g].wait()
            low = c * step
            total = total + times_transposed(
                upstream[:, low : low + step], out_vmem[g, :, low : low + step]
            )
        down = total.astype(jnp.bfloat16)
        down_ref[g] = down
        for c in range(CHUNKS):
            value_copies[c * groups + g].wait()
            low = c * step
            part_ref[g, :, low : low + step] = times_transposed(
                down, value_vmem[g, low : low + step, :]
            ).astype(jnp.bfloat16)


def source_kernel(ticks, *refs):
    rows = refs[:ticks]
    gain_ref, value_ref, normed_ref, values_ref = refs[ticks:]
    row_count = rows[0].shape[1]
    for t in range(ticks):
        scaled, inv_root = scaled_rows(rows[t][0])
        normed_ref[0, t * row_count : (t + 1) * row_count, :] = (scaled * gain_ref[0]).astype(
            jnp.bfloat16
        )
    values_ref[0] = jnp.dot(
        normed_ref[0], value_ref[0], preferred_element_type=jnp.float32
    ).astype(jnp.bfloat16)


def gradient_kernel(scale, ticks, *refs):
    def joined(some):
        return jnp.concatenate([ref[0] for ref in some], axis=0)

    upstream = joined(refs[:ticks])
    down = joined(refs[ticks : 2 * ticks])
    normed_ref, values_ref, value_ref, out_ref = refs[2 * ticks :]
    normed = normed_ref[0]
    values = values_ref[0]
    value_ref[0] = (transposed_times(normed, down) * scale).astype(jnp.bfloat16)
    out_ref[0] = (transposed_times(values, upstream) * scale).astype(jnp.bfloat16)


def layer_scratch(groups, value_mats, out_mats):
    return [
        pltpu.VMEM((groups,) + value_mats.shape[1:], value_mats.dtype),
        pltpu.VMEM((groups,) + out_mats.shape[1:], out_mats.dtype),
        pltpu.SemaphoreType.DMA((2, groups, CHUNKS)),
    ]


vmem_spec = pl.BlockSpec(memory_space=pltpu.VMEM)
any_spec = pl.BlockSpec(memory_space=pl.ANY)


smem_spec = pl.BlockSpec(memory_space=pltpu.SMEM)


def forward_parts(at_first, moved, entering, gains, value_mats, out_mats):
    groups = moved.shape[0]
    rows = jax.ShapeDtypeStruct(moved.shape, jnp.bfloat16)
    return pl.pallas_call(
        forward_kernel,
        out_shape=(rows, rows),
        in_specs=[smem_spec, vmem_spec, vmem_spec, vmem_spec, any_spec, any_spec],
        out_specs=(vmem_spec, vmem_spec),
        scratch_shapes=layer_scratch(groups, value_mats, out_mats),
        cost_estimate=pl.CostEstimate(
            flops=4 * moved.size * value_mats.shape[2],
            bytes_accessed=4 * groups * value_mats.shape[1] * value_mats.shape[2],
            transcendentals=0,
        ),
        name="forward_parts",
    )(at_first, moved, entering, gains, value_mats, out_mats)


def backward_parts(at_last, moved, outputs, ends, value_mats, out_mats):
    groups, row_count = moved.shape[:2]
    small = jax.ShapeDtypeStruct((groups, row_count, value_mats.shape[2]), jnp.bfloat16)
    large = jax.ShapeDtypeStruct(moved.shape, jnp.bfloat16)
    return pl.pallas_call(
        backward_kernel,
        out_shape=(large, large, small),
        in_specs=[smem_spec, vmem_spec, vmem_spec, vmem_spec, any_spec, any_spec],
        out_specs=(vmem_spec,) * 3,
        scratch_shapes=layer_scratch(groups, value_mats, out_mats),
        cost_estimate=pl.CostEstimate(
            flops=4 * moved.size * value_mats.shape[2],
            bytes_accessed=4 * groups * value_mats.shape[1] * value_mats.shape[2],
            transcendentals=0,
        ),
        name="backward_parts",
    )(at_last, moved, outputs, ends, value_mats, out_mats)


def source_values(sources, gains, value_mats):
    ticks = len(sources)
    groups, row_count, width = sources[0].shape
    features = value_mats.shape[2]
    whole = pl.BlockSpec((1, row_count, width), lambda g: (g, 0, 0))
    return pl.pallas_call(
        functools.partial(source_kernel, ticks),
        grid=(groups,),
        out_shape=(
            jax.ShapeDtypeStruct((groups, ticks * row_count, width), jnp.bfloat16),
            jax.ShapeDtypeStruct((groups, ticks * row_count, features), jnp.bfloat16),
        ),
        in_specs=[whole] * ticks
        + [
            pl.BlockSpec((1, 1, width), lambda g: (g, 0, 0)),
            pl.BlockSpec((1, width, features), lambda g: (g, 0, 0)),
        ],
        out_specs=(
            pl.BlockSpec((1, ticks * row_count, width), lambda g: (g, 0, 0)),
            pl.BlockSpec((1, ticks * row_count, features), lambda g: (g, 0, 0)),
        ),
        cost_estimate=pl.CostEstimate(
            flops=2 * ticks * row_count * groups * width * features,
            bytes_accessed=2 * groups * width * features,
            transcendentals=0,
        ),
        name="source_values",
    )(*sources, gains, value_mats)


def weight_gradients(scale, upstream, down, normed, values):
    ticks = len(upstream)
    groups, row_count, width = upstream[0].shape
    features = down[0].shape[2]
    step = width // CHUNKS
    wide = pl.BlockSpec((1, row_count, step), lambda g, c: (g, 0, c))
    narrow = pl.BlockSpec((1, row_count, features), lambda g, c: (g, 0, 0))
    return pl.pallas_call(
        functools.partial(gradient_kernel, scale, ticks),
        grid=(groups, CHUNKS),
        out_shape=(
            jax.ShapeDtypeStruct((groups, width, features), jnp.bfloat16),
            jax.ShapeDtypeStruct((groups, features, width), jnp.bfloat16),
        ),
        in_specs=[wide] * ticks
        + [narrow] * ticks
        + [
            pl.BlockSpec((1, ticks * row_count, step), lambda g, c: (g, 0, c)),
            pl.BlockSpec((1, ticks * row_count, features), lambda g, c: (g, 0, 0)),
        ],
        out_specs=(
            pl.BlockSpec((1, step, features), lambda g, c: (g, c, 0)),
            pl.BlockSpec((1, features, step), lambda g, c: (g, 0, c)),
        ),
        cost_estimate=pl.CostEstimate(
            flops=4 * ticks * row_count * groups * width * features,
            bytes_accessed=4 * groups * width * features,
            transcendentals=0,
        ),
        name="weight_gradients",
    )(*upstream, *down, normed, values)


def after(value, earlier):
    return lax.optimization_barrier((value, earlier))[0]


def body(
    w_value,
    w_out,
    norm_gain,
    saved_inputs,
    arriving,
    returning,
    fresh_rows,
    targets,
    fill_slots,
    read_slots,
):
    value_mats = w_value[0]
    out_mats = w_out[0]
    gains = norm_gain[0][:, None, :]
    saved = saved_inputs[0]
    fills = fill_slots[0]
    reads = read_slots[0]
    tick_count = fresh_rows.shape[0]
    slot_count = saved.shape[0]
    tok_rows = arriving.shape[2]
    all_rows = tok_rows * lax.axis_size("dp")
    section_index = lax.axis_index("section")
    last_section = lax.axis_size("section") - 1
    row_offset = lax.axis_index("dp") * tok_rows
    def own_rows(block):
        return lax.dynamic_slice_in_dim(block, row_offset, tok_rows, block.ndim - 2)

    def read_saved(tick_index):
        return jnp.stack([saved[reads[tick_index, group], group] for group in range(2)])

    never = jnp.zeros((1,), jnp.int32)
    at_first = (section_index == 0).astype(jnp.int32)[None]
    at_last = (section_index == last_section).astype(jnp.int32)[None]
    moved = all_replicas(arriving[0])
    first_two = all_replicas(after(jnp.stack([returning[0], read_saved(0)]), moved))
    returned, old_source = first_two[0], first_two[1]
    new_rows = replicas_of_section(after(fresh_rows[1:], moved), 0)
    entering, ends, outputs = moved[0], moved[0], moved

    inputs, sources, upstreams, downs = [], [], [], []
    gain_sums = jnp.zeros((2, gains.shape[2]), jnp.float32)
    for tick_index in range(tick_count):
        if tick_index > 0:
            moved = shifted(outputs, "section", 1)
            entering = new_rows[tick_index - 1]
            returned = shifted(gradients, "section", -1)
            if tick_index == 1:
                finished = replicas_of_section(
                    after(targets[: tick_count - 1], outputs), last_section
                )
            ends = finished[tick_index - 1]
            old_source = all_replicas(after(read_saved(tick_index), outputs))
        previous = outputs
        forward_part, activations = forward_parts(
            at_first if tick_index > 0 else never, moved, entering, gains, value_mats, out_mats
        )
        inputs.append(activations)
        outputs = (activations.astype(jnp.float32) + replica_sum(forward_part)).astype(
            jnp.bfloat16
        )
        source = old_source
        for earlier in range(tick_index + 1):
            same = fills[earlier] == reads[tick_index]
            source = jnp.where(same[:, None, None], inputs[earlier], source)
        sources.append(source)
        backward_part, cotangents, down = backward_parts(
            at_last if tick_index > 0 else never, returned, previous, ends, value_mats, out_mats
        )
        upstreams.append(cotangents)
        downs.append(down)
        pulled = replica_sum(backward_part)
        scaled, inv_root = scaled_rows(source)
        weighted = pulled * gains
        inner_mean = jnp.mean(weighted * scaled, axis=-1, keepdims=True)
        gradients = (
            cotangents.astype(jnp.float32) + inv_root * (weighted - scaled * inner_mean)
        ).astype(jnp.bfloat16)
        gain_sums = gain_sums + jnp.sum(pulled * scaled, axis=1)
    grad_scale = (tick_count * all_rows) ** (-0.5)
    normed, values = source_values(sources, gains, value_mats)
    grad_value, grad_out = weight_gradients(grad_scale, upstreams, downs, normed, values)
    slot_ids = jnp.arange(slot_count, dtype=jnp.int32)
    stash = saved
    for tick_index in range(tick_count):
        written = slot_ids[:, None] == fills[tick_index][None, :]
        stash = jnp.where(
            written[:, :, None, None], own_rows(inputs[tick_index])[None], stash
        )
    return (
        own_rows(outputs)[None],
        own_rows(gradients)[None],
        stash[None],
        grad_value[None],
        grad_out[None],
        (gain_sums * grad_scale)[None],
    )


def solution(mesh):
    in_specs = (
        P("section", None, None, "dp"),
        P("section", None, "dp", None),
        P("section", None, None),
        P("section", None, None, "dp", None),
        P("section", None, "dp", None),
        P("section", None, "dp", None),
        P(None, "dp", None),
        P(None, "dp", None),
        P("section", None, None),
        P("section", None, None),
    )
    out_specs = (
        P("section", None, "dp", None),
        P("section", None, "dp", None),
        P("section", None, None, "dp", None),
        P("section", None, None, "dp"),
        P("section", None, "dp", None),
        P("section", None, None),
    )
    return jax.shard_map(body, mesh=mesh, in_specs=in_specs, out_specs=out_specs, check_vma=False)
```
